32 devices in a mesh: groups: 2 (over x), chan: 8 (over z, y), space: 2 (over core).
Axes of the slice: x: 2, y: 2, z: 4, core: 2. Of those that a mesh axis runs over, the one named last changes fastest.
Arguments:
- cube: bfloat16 [32, 1024, 512], P(('groups', 'chan'), 'space'), parts along dimension 0, may hold values from -40 to 40
- beam_response: float32 [1024, 512], P(None, 'space'), may hold values from 0.1 to 1
- line_widths: float32 [5], replicated, may hold values from 0.6 to 3
Outputs:
- detection: bfloat16 [32, 1024, 512], P(('groups', 'chan'), 'space'), parts along dimension 0
The draws below stay inside these ranges and needn't reach their ends.
There are 2 independent parts, one for each index of `groups`. The reference program is written for one: setup_inputs(seed, part) draws one part's arguments, and reference() takes and returns one part's arrays. A program takes and returns all parts, laid end to end along the dimension named above; an argument that names none is the same for every part. Nothing has to cross between parts.
All inputs are finite; a program needn't handle non-finite values.
Results may differ from the reference program's by a relative error of at most 0.025.
Values may be sent and summed in bfloat16 or wider, within the bound.
A program may use at most 128 MiB of HBM per device.

```python
import math
import jax
import jax.numpy as jnp
from jax import lax

ROWS = 1024
COLS = 512
ORDER = 8
KERNELS = 5
HALO = 2
CHANNELS = 16


def draw_cube(key, part):
    keys = jax.random.split(jax.random.fold_in(key, 17), 2)
    rowpos = jnp.arange(ROWS, dtype=jnp.int32).astype(jnp.float32) / max(ROWS - 1, 1)
    row_scale = jnp.exp(math.log(3.0) * rowpos)
    col_scale = jnp.exp(jax.random.uniform(keys[1], (COLS,), jnp.float32, 0.0, math.log(3.3)))
    base = jnp.clip(jax.random.normal(keys[0], (CHANNELS, ROWS, COLS), jnp.float32), -4.0, 4.0)
    values = base * row_scale[None, :, None] * col_scale[None, None, :]
    return values.astype(jnp.bfloat16)


def shard_levels(rng, shape, cuts, smallest, high):
    factor_of, own = 1.0, jax.random.fold_in(rng, 6)
    for dim, parts in cuts:
        steps = jnp.exp(jax.random.uniform(jax.random.fold_in(own, dim), (parts,), jnp.float32, smallest / len(cuts), high / len(cuts)))
        factor_of = factor_of * jnp.repeat(steps, shape[dim] // parts).reshape([-1 if axis == dim else 1 for axis in range(len(shape))])
    return factor_of


def setup_inputs(seed: int = 0, part: int = 0) -> dict:
    arg_keys = jax.random.split(jax.random.key(seed), 4)
    part_splits = jax.random.split(jax.random.fold_in(arg_keys[3], part), 4)
    cube = draw_cube(jax.random.fold_in(jax.random.fold_in(arg_keys[3], part), 71), part)
    beam_response = jnp.clip(0.1 + 0.9 * jax.random.uniform(arg_keys[1], (ROWS, COLS), jnp.float32) ** shard_levels(arg_keys[1], (ROWS, COLS), ((1, 2),), -0.2, 0.2), 0.1, 1.0)
    line_widths = jnp.clip(jnp.exp(jax.random.uniform(arg_keys[2], (KERNELS,), jnp.float32, math.log(0.6), math.log(3.0))), 0.6, 3.0)
    return {"cube": cube, "beam_response": beam_response, "line_widths": line_widths}


def legendre_basis(channels):
    pos = jnp.arange(channels, dtype=jnp.int32).astype(jnp.float32)
    xval = -1.0 + (2.0 * pos + 1.0) / channels
    columns = [jnp.ones_like(xval), xval]
    for degree in range(1, ORDER):
        nxt = ((2.0 * degree + 1.0) * xval * columns[degree] - degree * columns[degree - 1]) / (degree + 1.0)
        columns.append(nxt)
    done = []
    for degree in range(ORDER + 1):
        vector = columns[degree]
        for prior in done:
            vector = vector - jnp.sum(prior * vector) * prior
        vector = vector / jnp.sqrt(jnp.sum(vector * vector))
        done.append(vector)
    return jnp.stack(done, axis=1)

def dft_tables(length):
    index = jnp.arange(length, dtype=jnp.int32)
    product = index[:, None] * index[None, :] % length
    phase = product.astype(jnp.float32) * (2.0 * math.pi / length)
    return (jnp.cos(phase).astype(jnp.bfloat16), jnp.sin(phase).astype(jnp.bfloat16))

def kernel_taps(widths, reach):
    offset = jnp.arange(-reach, reach + 1, dtype=jnp.int32).astype(jnp.float32)
    shape = jnp.exp(-offset[None, :] ** 2 / (2.0 * widths[:, None] ** 2))
    return (shape / jnp.sqrt(lax.optimization_barrier(jnp.sum(shape * shape, axis=1, keepdims=True)))).astype(jnp.bfloat16)

def band_matrix(taps, count, reach):
    chans = jnp.arange(count, dtype=jnp.int32)
    padded = jnp.arange(count + 2 * reach, dtype=jnp.int32)
    offset = padded[None, :] - chans[:, None]
    picks = jnp.arange(2 * reach + 1, dtype=jnp.int32)
    onehot = (offset[:, :, None] == picks[None, None, :]).astype(jnp.float32)
    return jnp.einsum('kj,cmj->kcm', taps.astype(jnp.float32), onehot).astype(jnp.bfloat16)

def product(form, left, right):
    return jnp.einsum(form, left.astype(jnp.float32), right.astype(jnp.float32), precision=lax.Precision.HIGHEST)

def reference(cube, beam_response, line_widths):
    chans, rows, cols = cube.shape
    basis = legendre_basis(chans)
    values = cube.reshape(chans, rows * cols).astype(jnp.float32)
    coeffs = jnp.dot(basis.T, values, precision=lax.Precision.HIGHEST)
    line = (values - jnp.dot(basis, coeffs, precision=lax.Precision.HIGHEST)).astype(jnp.bfloat16)
    line = line.reshape(chans, rows, cols)
    ccos, csin = dft_tables(cols)
    rcos, rsin = dft_tables(rows)
    xreal = product('crq,qm->crm', line, ccos).astype(jnp.bfloat16)
    ximag = (-product('crq,qm->crm', line, csin)).astype(jnp.bfloat16)
    yreal = product('ur,crm->cum', rcos, xreal) + product('ur,crm->cum', rsin, ximag)
    yimag = product('ur,crm->cum', rcos, ximag) - product('ur,crm->cum', rsin, xreal)
    zreal = (yreal * beam_response[None]).astype(jnp.bfloat16)
    zimag = (yimag * beam_response[None]).astype(jnp.bfloat16)
    wreal = (product('ur,crm->cum', rcos, zreal) - product('ur,crm->cum', rsin, zimag)).astype(jnp.bfloat16)
    wimag = (product('ur,crm->cum', rcos, zimag) + product('ur,crm->cum', rsin, zreal)).astype(jnp.bfloat16)
    smooth = (product('crq,qm->crm', wreal, ccos) - product('crq,qm->crm', wimag, csin)) / (rows * cols)
    smooth = smooth.astype(jnp.bfloat16).reshape(chans, rows * cols)
    taps = kernel_taps(line_widths, HALO)
    band = band_matrix(taps, chans, HALO)
    padded = jnp.pad(smooth, ((HALO, HALO), (0, 0)))
    best = None
    for kernel in range(KERNELS):
        filtered = jnp.dot(band[kernel], padded, preferred_element_type=jnp.float32)
        noise = jnp.sqrt(lax.optimization_barrier(jnp.mean(filtered * filtered, axis=1)) + 1e-06)
        ratio = filtered / noise[:, None]
        best = ratio if best is None else jnp.maximum(best, ratio)
    return best.astype(jnp.bfloat16).reshape(chans, rows, cols)
```

```python
import functools
import math

import jax
import jax.numpy as jnp
import numpy as np
from jax import lax
from jax.experimental import pallas as pl
from jax.experimental.pallas import tpu as pltpu
from jax.sharding import PartitionSpec as P

ORDER = 8
HALO = 2
BF = jnp.bfloat16
F32 = jnp.float32


def residual_matrix(channels):
    xval = -1.0 + (2.0 * np.arange(channels) + 1.0) / channels
    cols = [np.ones_like(xval), xval]
    for degree in range(1, ORDER):
        cols.append(
            ((2.0 * degree + 1.0) * xval * cols[degree] - degree * cols[degree - 1])
            / (degree + 1.0)
        )
    basis, _ = np.linalg.qr(np.stack(cols, axis=1))
    return np.eye(channels) - basis @ basis.T


def subtract_kernel(even, odd, x_ref, o_ref):
    channels, _, cols = x_ref.shape
    half = channels // 2
    for lane in range(0, cols, 128):
        lanes = pl.ds(lane, 128)
        sums, diffs = [], []
        for i in range(half):
            lo = x_ref[i, :, lanes].astype(F32)
            hi = x_ref[channels - 1 - i, :, lanes].astype(F32)
            sums.append(lo + hi)
            diffs.append(lo - hi)
        for c in range(half):
            p = sum(float(even[c, i]) * sums[i] for i in range(half))
            m = sum(float(odd[c, i]) * diffs[i] for i in range(half))
            o_ref[c, :, lanes] = (p + m).astype(o_ref.dtype)
            o_ref[channels - 1 - c, :, lanes] = (p - m).astype(o_ref.dtype)


def subtract(spread):
    channels, rows, cols = spread.shape
    half = channels // 2
    m = residual_matrix(channels)
    even = 0.5 * (m[:half, :half] + m[:half, ::-1][:, :half])
    odd = 0.5 * (m[:half, :half] - m[:half, ::-1][:, :half])
    block = 16 if rows % 16 == 0 else rows
    spec = pl.BlockSpec((channels, block, cols), lambda i: (0, i, 0))
    return pl.pallas_call(
        functools.partial(subtract_kernel, even, odd),
        grid=(rows // block,),
        in_specs=[spec],
        out_specs=spec,
        out_shape=jax.ShapeDtypeStruct(spread.shape, BF),
        cost_estimate=pl.CostEstimate(
            flops=channels * channels * rows * cols,
            bytes_accessed=4 * spread.size,
            transcendentals=0,
        ),
        name="subtract",
    )(spread)


def tables(left, right, length):
    phase = (left[:, None] * right[None, :] % length) * (2.0 * math.pi / length)
    return (
        jnp.asarray(np.cos(phase), dtype=BF),
        jnp.asarray(np.sin(phase), dtype=BF),
    )


def kernel_taps(widths, reach):
    offset = jnp.arange(-reach, reach + 1, dtype=jnp.int32).astype(F32)
    shape = jnp.exp(-offset[None, :] ** 2 / (2.0 * widths[:, None] ** 2))
    return (shape / jnp.sqrt(jnp.sum(shape * shape, axis=1, keepdims=True))).astype(BF)


def mm(a, b, dims=((1,), (0,))):
    return lax.dot_general(a, b, (dims, ((), ())), preferred_element_type=F32)


def flip(n):
    i = np.arange(n)
    return jnp.asarray((i[:, None] + i[None, :]) % n == 0, dtype=BF)


def swap(x, axis):
    count = lax.axis_size(axis)
    return lax.ppermute(x, axis, [(i, (i + 1) % count) for i in range(count)])


def local(cube, beam, line_widths):
    local_chans, local_rows, cols = cube.shape
    nchan, nspace = lax.axis_size("chan"), lax.axis_size("space")
    channels = local_chans * nchan
    rows = local_rows * nspace
    half = cols // nspace
    mine = lax.axis_index("space")
    other = swap(beam.astype(BF), "space")
    flipped_cols = mm(other, flip(half)).astype(BF)
    first = jnp.arange(half) == 0
    flipped_cols = jnp.where(first[None, :], beam[:, :1].astype(BF), flipped_cols)
    flipped = mm(flip(rows), flipped_cols)
    sym = (0.5 * (beam + flipped)).reshape(rows // 2, 2, half)
    beam_even, beam_odd = sym[:, 0], sym[:, 1]

    spread = lax.all_to_all(cube, "chan", split_axis=1, concat_axis=0, tiled=True)
    line = subtract(spread)
    share = local_rows // nchan
    pairs = channels // 2
    packed = line.reshape(pairs, 2, share, cols)
    a = packed[:, 0].reshape(pairs * share, cols)
    b = packed[:, 1].reshape(pairs * share, cols)
    index = np.arange(cols)
    ccos, csin = tables(index, index, cols)
    xr = (mm(a, ccos) + mm(b, csin)).astype(BF)
    xi = (mm(b, ccos) - mm(a, csin)).astype(BF)
    parts = [
        jnp.concatenate([xr[:, s * half:(s + 1) * half], xi[:, s * half:(s + 1) * half]], axis=1)
        .reshape(nchan, -1, 2 * half)
        for s in range(nspace)
    ]
    sent = jnp.stack(parts, axis=1).reshape(nchan * nspace, -1, 2 * half)
    got = lax.all_to_all(sent, ("chan", "space"), split_axis=0, concat_axis=0, tiled=True)
    got = got.reshape(nchan, nspace, share, 2 * half)
    top = got[:, 0].reshape(local_rows, 2 * half).astype(F32)
    low = got[:, 1].reshape(local_rows, 2 * half).astype(F32)
    halfrow = rows // 2
    r = np.arange(halfrow)
    ecos, esin = tables(2 * r, r, rows)
    ocos, osin = tables(2 * r + 1, r, rows)

    def filt(x, cos, sin, response):
        p, q = mm(cos, x), mm(sin, x)
        zr = ((p[:, :half] + q[:, half:]) * response).astype(BF)
        zi = ((p[:, half:] - q[:, :half]) * response).astype(BF)
        z = jnp.concatenate([zr, zi], axis=1)
        t = ((0,), (0,))
        p, q = mm(cos, z, t), mm(sin, z, t)
        return jnp.concatenate([p[:, :half] - q[:, half:], p[:, half:] + q[:, :half]], axis=1)

    we = filt((top + low).astype(BF), ecos, esin, beam_even)
    wo = filt((top - low).astype(BF), ocos, osin, beam_odd)
    sign = jnp.where(mine == 0, 1.0, -1.0).astype(F32)
    own = (we + sign * wo).astype(BF)
    away = swap((we - sign * wo).astype(BF), "space")
    def back(w, which):
        c = lax.dynamic_slice_in_dim(ccos, which * half, half, 0)
        s = lax.dynamic_slice_in_dim(csin, which * half, half, 0)
        wr, wi = w[:, :half], w[:, half:]
        return mm(wr, c) - mm(wi, s), mm(wi, c) + mm(wr, s)

    own_a, own_b = back(own, mine)
    far_a, far_b = back(away, 1 - mine)
    scale = 1.0 / (rows * cols)
    smooth = jnp.stack(
        [((own_a + far_a) * scale).astype(BF), ((own_b + far_b) * scale).astype(BF)], axis=0
    )
    up = [(i, i + 1) for i in range(nchan - 1)]
    down = [(i + 1, i) for i in range(nchan - 1)]
    low_halo = lax.ppermute(smooth[local_chans - HALO:], "chan", up)
    high_halo = lax.ppermute(smooth[:HALO], "chan", down)
    chans = [x[i] for x in (low_halo, smooth, high_halo) for i in range(x.shape[0])]
    taps = kernel_taps(line_widths, HALO).astype(F32)
    kernels = taps.shape[0]

    def responses(c):
        s = [x.astype(F32) for x in chans[c:c + 2 * HALO + 1]]
        return [sum(taps[k, j] * s[j] for j in range(2 * HALO + 1)) for k in range(kernels)]

    squares = jnp.stack(
        [jnp.sum(f * f) for c in range(local_chans) for f in responses(c)]
    )
    totals = jnp.broadcast_to(squares[None, :], (8, squares.shape[0]))
    totals = (totals + swap(totals, "space"))[0]
    inv = 1.0 / jnp.sqrt(totals / (rows * cols) + 1e-06)
    out = []
    for c in range(local_chans):
        scaled = [f * inv[c * kernels + k] for k, f in enumerate(responses(c))]
        out.append(functools.reduce(jnp.maximum, scaled).astype(BF))
    return jnp.stack(out, axis=0)


def solution(mesh):
    in_specs = (P(("groups", "chan"), "space", None), P(None, "space"), P())
    out_specs = P(("groups", "chan"), "space", None)
    return jax.shard_map(local, mesh=mesh, in_specs=in_specs, out_specs=out_specs, check_vma=False)
```

```python
import functools
import math

import jax
import jax.numpy as jnp
import numpy as np
from jax import lax
from jax.experimental import pallas as pl
from jax.experimental.pallas import tpu as pltpu
from jax.sharding import PartitionSpec as P


ORDER = 8
HALO = 2
CHUNKS = 4
BF = jnp.bfloat16
F32 = jnp.float32


def residual_matrix(channels):
    xval = -1.0 + (2.0 * np.arange(channels) + 1.0) / channels
    cols = [np.ones_like(xval), xval]
    for degree in range(1, ORDER):
        cols.append(
            ((2.0 * degree + 1.0) * xval * cols[degree] - degree * cols[degree - 1])
            / (degree + 1.0)
        )
    basis, _ = np.linalg.qr(np.stack(cols, axis=1))
    return np.eye(channels) - basis @ basis.T


def subtract_kernel(even, odd, x_ref, o_ref):
    channels, _, cols = x_ref.shape
    half = channels // 2
    for lane in range(0, cols, 128):
        lanes = pl.ds(lane, 128)
        sums, diffs = [], []
        for i in range(half):
            lo = x_ref[i, :, lanes].astype(F32)
            hi = x_ref[channels - 1 - i, :, lanes].astype(F32)
            sums.append(lo + hi)
            diffs.append(lo - hi)
        for c in range(half):
            p = sum(float(even[c, i]) * sums[i] for i in range(half))
            m = sum(float(odd[c, i]) * diffs[i] for i in range(half))
            o_ref[c, :, lanes] = (p + m).astype(o_ref.dtype)
            o_ref[channels - 1 - c, :, lanes] = (p - m).astype(o_ref.dtype)


def subtract(spread):
    channels, rows, cols = spread.shape
    half = channels // 2
    m = residual_matrix(channels)
    even = 0.5 * (m[:half, :half] + m[:half, ::-1][:, :half])
    odd = 0.5 * (m[:half, :half] - m[:half, ::-1][:, :half])
    block = 16 if rows % 16 == 0 else rows
    spec = pl.BlockSpec((channels, block, cols), lambda i: (0, i, 0))
    return pl.pallas_call(
        functools.partial(subtract_kernel, even, odd),
        grid=(rows // block,),
        in_specs=[spec],
        out_specs=spec,
        out_shape=jax.ShapeDtypeStruct(spread.shape, BF),
        cost_estimate=pl.CostEstimate(
            flops=channels * channels * rows * cols,
            bytes_accessed=4 * spread.size,
            transcendentals=0,
        ),
        name="subtract",
    )(spread)


def tables(left, right, length):
    phase = (left[:, None] * right[None, :] % length) * (2.0 * math.pi / length)
    return (
        jnp.asarray(np.cos(phase), dtype=BF),
        jnp.asarray(np.sin(phase), dtype=BF),
    )


def kernel_taps(widths, reach):
    offset = jnp.arange(-reach, reach + 1, dtype=jnp.int32).astype(F32)
    shape = jnp.exp(-offset[None, :] ** 2 / (2.0 * widths[:, None] ** 2))
    return (shape / jnp.sqrt(jnp.sum(shape * shape, axis=1, keepdims=True))).astype(BF)


def mm(a, b, dims=((1,), (0,))):
    return lax.dot_general(a, b, (dims, ((), ())), preferred_element_type=F32)


def split(x):
    high = lax.reduce_precision(x, 8, 7)
    return high.astype(BF), (x - high).astype(BF)


def mm_left(a, b, dims=((1,), (0,))):
    high, low = split(a)
    return mm(high, b, dims) + mm(low, b, dims)


def mm_right(a, b, dims=((1,), (0,))):
    high, low = split(b)
    return mm(a, high, dims) + mm(a, low, dims)


def flip(n):
    i = np.arange(n)
    return jnp.asarray((i[:, None] + i[None, :]) % n == 0, dtype=BF)


def windows(refs, where):
    low, mid, high = [[ref[i, where[0], where[1]].astype(F32) for i in range(2)] for ref in refs]
    s = low + mid + high
    return [(s[c + 2], s[c + 1] + s[c + 3], s[c] + s[c + 4]) for c in range(2)]


def for_chunks(parity_ref, refs, body):
    smooth, near, far = refs[:CHUNKS], refs[CHUNKS:2 * CHUNKS], refs[2 * CHUNKS:3 * CHUNKS]
    for odd in range(2):

        @pl.when(parity_ref[0] == odd)
        def _():
            for n in range(CHUNKS):
                low, high = (near[n], far[n]) if odd else (far[n], near[n])
                rows = smooth[n].shape[1]

                def tile(i, carry, n=n, low=low, high=high, rows=rows):
                    body((low, smooth[n], high), i * 16, n * rows)
                    return carry

                lax.fori_loop(0, rows // 16, tile, 0)


def stats_kernel(parity_ref, taps_ref, *refs):
    out = refs[-1]
    kernels = taps_ref.shape[0]
    out[...] = jnp.zeros_like(out)

    def body(blocks, row, base):
        acc = [None] * (2 * kernels)
        for lane in range(0, blocks[1].shape[2], 128):
            w = windows(blocks, (pl.ds(pl.multiple_of(row, 16), 16), pl.ds(lane, 128)))
            for c in range(2):
                for k in range(kernels):
                    f = sum(taps_ref[k, j] * w[c][j] for j in range(HALO + 1))
                    n = c * kernels + k
                    acc[n] = f * f if acc[n] is None else acc[n] + f * f
        for n in range(2 * kernels):
            out[n] += acc[n]

    for_chunks(parity_ref, refs, body)


def best_kernel(parity_ref, taps_ref, *refs):
    out = refs[-1]
    kernels = taps_ref.shape[0] // 2

    def body(blocks, row, base):
        for lane in range(0, blocks[1].shape[2], 128):
            lanes = pl.ds(lane, 128)
            w = windows(blocks, (pl.ds(pl.multiple_of(row, 16), 16), lanes))
            for c in range(2):
                best = None
                for k in range(kernels):
                    f = sum(taps_ref[c * kernels + k, j] * w[c][j] for j in range(HALO + 1))
                    best = f if best is None else jnp.maximum(best, f)
                out[c, pl.ds(pl.multiple_of(base + row, 16), 16), lanes] = best.astype(out.dtype)

    for_chunks(parity_ref, refs, body)


def filter_call(kernel, shape, dtype, name, parity, taps, blocks):
    size = sum(b.size for b in blocks)
    return pl.pallas_call(
        kernel,
        in_specs=[pl.BlockSpec(memory_space=pltpu.SMEM)] * 2
        + [pl.BlockSpec(memory_space=pltpu.VMEM)] * len(blocks),
        out_specs=pl.BlockSpec(memory_space=pltpu.VMEM),
        out_shape=jax.ShapeDtypeStruct(shape, dtype),
        cost_estimate=pl.CostEstimate(flops=20 * size, bytes_accessed=3 * size, transcendentals=0),
        name=name,
    )(parity, taps, *blocks)


def swap(x, axis):
    count = lax.axis_size(axis)
    return lax.ppermute(x, axis, [(i, (i + 1) % count) for i in range(count)])


def local(cube, beam, line_widths):
    local_chans, local_rows, cols = cube.shape
    nchan, nspace = lax.axis_size("chan"), lax.axis_size("space")
    channels = local_chans * nchan
    rows = local_rows * nspace
    half = cols // nspace
    mine = lax.axis_index("space")
    other = swap(beam, "space")
    flipped_cols = mm_left(other, flip(half))
    first = jnp.arange(half) == 0
    flipped_cols = jnp.where(first[None, :], beam[:, :1], flipped_cols)
    flipped = mm_right(flip(rows), flipped_cols)
    sym = (0.5 * (beam + flipped)).reshape(rows // 2, 2, half)
    beam_even, beam_odd = sym[:, 0], sym[:, 1]

    spread = lax.all_to_all(cube, "chan", split_axis=1, concat_axis=0, tiled=True)
    line = subtract(spread)
    share = local_rows // nchan
    pairs = channels // 2
    packed = line.reshape(pairs, 2, share, cols)
    a = packed[:, 0].reshape(pairs * share, cols)
    b = packed[:, 1].reshape(pairs * share, cols)
    index = np.arange(cols)
    ccos, csin = tables(index, index, cols)
    xr = (mm(a, ccos) + mm(b, csin)).astype(BF)
    xi = (mm(b, ccos) - mm(a, csin)).astype(BF)
    parts = [
        jnp.concatenate([xr[:, s * half:(s + 1) * half], xi[:, s * half:(s + 1) * half]], axis=1)
        .reshape(nchan, -1, 2 * half)
        for s in range(nspace)
    ]
    sent = jnp.stack(parts, axis=1).reshape(nchan * nspace, -1, 2 * half)
    got = lax.all_to_all(sent, ("chan", "space"), split_axis=0, concat_axis=0, tiled=True)
    got = got.reshape(nchan, nspace, share, 2 * half)
    top = got[:, 0].reshape(local_rows, 2 * half).astype(F32)
    low = got[:, 1].reshape(local_rows, 2 * half).astype(F32)
    halfrow = rows // 2
    r = np.arange(halfrow)
    ecos, esin = tables(2 * r, r, rows)
    ocos, osin = tables(2 * r + 1, r, rows)

    def filt(x, cos, sin, response):
        p, q = mm_right(cos, x), mm_right(sin, x)
        zr = (p[:, :half] + q[:, half:]) * response
        zi = (p[:, half:] - q[:, :half]) * response
        z = jnp.concatenate([zr, zi], axis=1)
        t = ((0,), (0,))
        p, q = mm_right(cos, z, t), mm_right(sin, z, t)
        return jnp.concatenate([p[:, :half] - q[:, half:], p[:, half:] + q[:, :half]], axis=1)

    we = filt(top + low, ecos, esin, beam_even)
    wo = filt(top - low, ocos, osin, beam_odd)
    sign = jnp.where(mine == 0, 1.0, -1.0).astype(F32)
    own = we + sign * wo
    away = swap(we - sign * wo, "space")
    def back(w, which):
        c = lax.dynamic_slice_in_dim(ccos, which * half, half, 0)
        s = lax.dynamic_slice_in_dim(csin, which * half, half, 0)
        wr, wi = w[:, :half], w[:, half:]
        return mm_left(wr, c) - mm_left(wi, s), mm_left(wi, c) + mm_left(wr, s)

    scale = 1.0 / (rows * cols)
    chunk = local_rows // CHUNKS
    trade = [(i, i ^ 1) for i in range(nchan)]
    onward = [
        (i, i + 2 if i % 2 == 0 else i - 2)
        for i in range(nchan)
        if 0 <= (i + 2 if i % 2 == 0 else i - 2) < nchan
    ]
    smooth, near, far = [], [], []
    for n in range(CHUNKS):
        part = slice(n * chunk, (n + 1) * chunk)
        own_a, own_b = back(own[part], mine)
        far_a, far_b = back(away[part], 1 - mine)
        pair = jnp.stack(
            [((own_a + far_a) * scale).astype(BF), ((own_b + far_b) * scale).astype(BF)]
        )
        smooth.append(pair)
        near.append(lax.ppermute(pair, "chan", trade))
        far.append(lax.ppermute(near[-1], "chan", onward))
    taps = kernel_taps(line_widths, HALO).astype(F32)[:, HALO:]
    kernels = taps.shape[0]
    parity = (lax.axis_index("chan") % 2).astype(jnp.int32).reshape(1)
    blocks = smooth + near + far
    acc = filter_call(
        stats_kernel, (local_chans * kernels, 16, 128), F32, "stats", parity, taps, blocks
    )
    squares = jnp.sum(acc, axis=(1, 2))
    totals = jnp.broadcast_to(squares[None, :], (8, squares.shape[0]))
    totals = (totals + swap(totals, "space"))[0]
    noise = jnp.sqrt(totals / (rows * cols) + 1e-06)
    scaled = jnp.tile(taps, (local_chans, 1)) / noise[:, None]
    return filter_call(best_kernel, cube.shape, BF, "best", parity, scaled, blocks)


def solution(mesh):
    in_specs = (P(("groups", "chan"), "space", None), P(None, "space"), P())
    out_specs = P(("groups", "chan"), "space", None)
    return jax.shard_map(local, mesh=mesh, in_specs=in_specs, out_specs=out_specs, check_vma=False)
```
